256 devices in a mesh: section: 8 (over y_hi, x), tensor: 16 (over z, core), dp: 2 (over y_lo).
Axes of the slice: x: 4, y: 4 (y_hi: 2, y_lo: 2; y = y_hi * 2 + y_lo), z: 8, core: 2. Of those that a mesh axis runs over, the one named last changes fastest.
Arguments:
- dec_queries: bfloat16 [8, 4, 512, 16384], P('section', 'dp', None, 'tensor'), may hold values from -8 to 8
- enc_keys: bfloat16 [8, 4, 512, 16384], P('section', 'dp', None, 'tensor'), may hold values from -4 to 4
- enc_values: bfloat16 [8, 4, 512, 16384], P('section', 'dp', None, 'tensor'), may hold values from -4 to 4
- out_grad: bfloat16 [8, 4, 512, 16384], P('section', 'dp', None, 'tensor'), may hold values from -15 to 15
- key_weight: bfloat16 [8, 1024, 16384], P('section', None, 'tensor'), may hold values from -0.1875 to 0.1875
- value_weight: bfloat16 [8, 1024, 16384], P('section', None, 'tensor'), may hold values from -0.1875 to 0.1875
- enc_hidden: float32 [4, 512, 1024], P('dp', 'section', 'tensor'), may hold values from -2 to 2, as said below
- enc_gain: float32 [1024], P('tensor'), may hold values from 0.1 to 1.9
Outputs:
- enc_input_grad: float32 [4, 512, 1024], P('dp', 'section', 'tensor')
The draws below stay inside these ranges and needn't reach their ends.
Inputs may be any that keep to these rules, and one draw needn't show every extreme that they name: `enc_hidden`: every entry's magnitude is at least 0.25.
All inputs are finite; a program needn't handle non-finite values.
Results may differ from the reference program's by a relative error of at most 0.0041.
Values sent between devices are 32-bit elements; how exact they have to be, the bound alone decides.
A program may use at most 128 MiB of HBM per device.

```python
import jax
import jax.numpy as jnp
from jax import lax

D = 1024
DK = 128
DEC = 512
ENC = 512
HEADS = 128
INNER = 16384
SECTIONS = 8
SEQS = 4


def shared_rows(key):
    return jnp.clip(jax.random.normal(jax.random.fold_in(key, 12), (SECTIONS, SEQS, 1, INNER), jnp.float32), -4.0, 4.0)


def aligned_spot(key):
    return jax.random.randint(jax.random.fold_in(key, 13), (), 0, ENC).astype(jnp.int32)


def draw_enc_keys(key, part):
    base = jnp.clip(jax.random.normal(jax.random.fold_in(key, 11), (SECTIONS, SEQS, ENC, INNER), jnp.float32), -4.0, 4.0)
    zero = jnp.zeros((), jnp.int32)
    base = lax.dynamic_update_slice(base, shared_rows(key), (zero, zero, aligned_spot(key), zero))
    return base.astype(jnp.bfloat16)


def draw_dec_queries(key, part):
    base = 0.1 * jnp.clip(jax.random.normal(jax.random.fold_in(key, 22), (SECTIONS, SEQS, DEC, INNER), jnp.float32), -6.0, 6.0)
    return base.astype(jnp.bfloat16)


def draw_enc_hidden(key, part):
    shape = (SEQS, ENC, D)
    own_sign = jnp.where(jax.random.bernoulli(jax.random.fold_in(key, 31), 0.5, shape), 1.0, -1.0)
    magnitude = jax.random.uniform(jax.random.fold_in(key, 36), shape, jnp.float32, 0.25, 2.0)
    sign = own_sign
    return (sign * magnitude).astype(jnp.float32)


def levels(key, dims, cuts, smallest, high):
    factor_of, own = 1.0, jax.random.fold_in(key, 6)
    for position, parts in cuts:
        draws = jnp.exp(jax.random.uniform(jax.random.fold_in(own, position), (parts,), jnp.float32, smallest / len(cuts), high / len(cuts)))
        factor_of = factor_of * jnp.repeat(draws, dims[position] // parts).reshape([-1 if axis == position else 1 for axis in range(len(dims))])
    return factor_of


def normal_values(rng, extent, spread, most, shards=(), kind=jnp.bfloat16):
    values = jax.random.normal(rng, extent, jnp.float32) * spread
    if len(shards) > 0:
        values = levels(rng, extent, shards, -0.22, 0.18) * values
    return jnp.clip(values, min=-most, max=most).astype(kind)


def setup_inputs(seed: int = 0) -> dict:
    seeds = jax.random.split(jax.random.key(seed), 9)
    return {
        "dec_queries": draw_dec_queries(jax.random.fold_in(seeds[8], 71), 0),
        "enc_keys": draw_enc_keys(jax.random.fold_in(seeds[8], 71), 0),
        "enc_values": normal_values(seeds[2], (SECTIONS, SEQS, ENC, INNER), 1.0, 4.0, ((0, 8), (1, 2), (3, 16))),
        "out_grad": normal_values(seeds[3], (SECTIONS, SEQS, DEC, INNER), 3.0, 15.0, ((0, 8), (1, 2), (3, 16))),
        "key_weight": normal_values(seeds[4], (SECTIONS, D, INNER), D ** -0.5, 0.1875, ((0, 8), (2, 16))),
        "value_weight": normal_values(seeds[5], (SECTIONS, D, INNER), D ** -0.5, 0.1875, ((0, 8), (2, 16))),
        "enc_hidden": draw_enc_hidden(jax.random.fold_in(seeds[8], 71), 0),
        "enc_gain": jnp.clip(1.0 + 0.18 * jax.random.normal(seeds[7], (D,), jnp.float32), 0.1, 1.9),
    }


def attention_grads(query, keyset, valueset, gradset):
    query_heads = query.reshape(DEC, HEADS, DK).astype(jnp.float32)
    key_heads = keyset.reshape(ENC, HEADS, DK).astype(jnp.float32)
    value_heads = valueset.reshape(ENC, HEADS, DK).astype(jnp.float32)
    grad_heads = gradset.reshape(DEC, HEADS, DK).astype(jnp.float32)
    scores = jnp.einsum('qhd,khd->hqk', query_heads, key_heads)
    shifted = jnp.exp(scores - lax.optimization_barrier(jnp.max(scores, axis=-1, keepdims=True)))
    attn_probs = shifted / lax.optimization_barrier(jnp.sum(shifted, axis=-1, keepdims=True))
    probs_low = lax.optimization_barrier(attn_probs.astype(jnp.bfloat16)).astype(jnp.float32)
    attended = jnp.einsum('hqk,khd->qhd', probs_low, value_heads)
    row_dot = lax.optimization_barrier(jnp.sum(grad_heads * attended, axis=-1))
    value_grad = jnp.einsum('hqk,qhd->khd', probs_low, grad_heads).astype(jnp.bfloat16)
    prob_grad = jnp.einsum('qhd,khd->hqk', grad_heads, value_heads)
    score_grad = attn_probs * (prob_grad - jnp.transpose(row_dot)[:, :, None])
    score_low = lax.optimization_barrier(score_grad.astype(jnp.bfloat16)).astype(jnp.float32)
    key_grad = jnp.einsum('hqk,qhd->khd', score_low, query_heads).astype(jnp.bfloat16)
    return (key_grad.reshape(ENC, HEADS * DK), value_grad.reshape(ENC, HEADS * DK))

def reference(dec_queries, enc_keys, enc_values, out_grad, key_weight, value_weight, enc_hidden, enc_gain):

    def section_term(pieces):
        query, keyset, valueset, gradset, weight_k, weight_v = pieces

        def seq_term(inner):
            key_grad, value_grad = attention_grads(inner[0], inner[1], inner[2], inner[3])
            first = jnp.dot(key_grad, jnp.transpose(weight_k), preferred_element_type=jnp.float32)
            second = jnp.dot(value_grad, jnp.transpose(weight_v), preferred_element_type=jnp.float32)
            return first + second
        return lax.map(seq_term, (query, keyset, valueset, gradset))
    terms = lax.map(section_term, (dec_queries, enc_keys, enc_values, out_grad, key_weight, value_weight))
    enc_grad = lax.optimization_barrier(jnp.sum(terms, axis=0))
    scaled = enc_gain * enc_grad
    square_total = lax.optimization_barrier(jnp.sum(enc_hidden * enc_hidden, axis=-1))
    cross_total = lax.optimization_barrier(jnp.sum(scaled * enc_hidden, axis=-1))
    inverse = lax.rsqrt(square_total / D + 1e-06)
    return scaled * inverse[..., None] - enc_hidden * (cross_total * inverse * inverse * inverse / D)[..., None]
```

```python
import functools

import jax
import jax.numpy as jnp
from jax import lax
from jax.experimental import pallas as pl
from jax.experimental.pallas import tpu as pltpu
from jax.sharding import PartitionSpec as P

D = 1024
DK = 128
EPS = 1e-06
F32 = jnp.float32
BF16 = jnp.bfloat16
MESH = pl.DeviceIdType.MESH

NSEQ = 2
HEADS = 8
ROWS = 512
NJ = 4
CW = D // NJ
NT = (((1,), (1,)), ((), ()))
NN = (((1,), (0,)), ((), ()))


def dot(a, b, dims, **kw):
    return lax.dot_general(a, b, dims, preferred_element_type=F32, **kw)


def kernel(
    q_hbm, k_hbm, v_hbm, g_hbm, wk_hbm, wv_hbm, hid_ref, gain_ref, out_ref,
    qs, ks, vs, gs, wks, wvs, kg, vg,
    part, d2dr, acc, r1, fin, xs, yr, zs, zr, cs, cr, hs, hg, gh, crossp, osend, orecv,
    in_sem, w_sem, d2d_s, d2d_r, x_s, x_r, y_s, y_r, z_s, z_r, c_s, c_r, h_s, h_r, o_s, o_r,
):
    section = lax.axis_index("section")
    tensor = lax.axis_index("tensor")
    yh, x = section // 4, section % 4
    z, c = tensor // 2, tensor % 2
    xp, xm, x2 = (x + 1) % 4, (x + 3) % 4, (x + 2) % 4
    to_core = {"tensor": z * 2 + (1 - c)}
    to_xp = {"section": yh * 4 + xp}
    to_xm = {"section": yh * 4 + xm}
    to_y = {"section": (1 - yh) * 4 + x}

    def loads(i):
        b, h = i // HEADS, i % HEADS
        cols = pl.ds(pl.multiple_of(h * DK, DK), DK)
        pairs = ((k_hbm, ks), (q_hbm, qs), (v_hbm, vs), (g_hbm, gs))
        return [
            pltpu.make_async_copy(src.at[0, b, :, cols], dst.at[i], in_sem.at[i, n])
            for n, (src, dst) in enumerate(pairs)
        ]

    def start_loads(i, _):
        for copy in loads(i):
            copy.start()
        return 0

    wcopies = [
        pltpu.make_async_copy(wk_hbm.at[0], wks, w_sem.at[0]),
        pltpu.make_async_copy(wv_hbm.at[0], wvs, w_sem.at[1]),
    ]
    lax.fori_loop(0, HEADS, start_loads, 0)
    for copy in wcopies:
        copy.start()
    lax.fori_loop(HEADS, NSEQ * HEADS, start_loads, 0)

    barrier = pltpu.get_barrier_semaphore()
    for peer in (to_xp, to_xm, to_y):
        pl.semaphore_signal(barrier, inc=1, device_id=peer, device_id_type=MESH)

    def greet(d, _):
        peer = {"tensor": (tensor + d) % 16}
        pl.semaphore_signal(barrier, inc=1, device_id=peer, device_id_type=MESH)
        return 0

    lax.fori_loop(1, 16, greet, 0)

    def send(src, dst, s, r, peer):
        return pltpu.make_async_remote_copy(
            src_ref=src, dst_ref=dst, send_sem=s, recv_sem=r, device_id=peer, device_id_type=MESH
        )

    def d2d_copy(b, j):
        return send(
            part.at[b, j, :, 1 - c], d2dr.at[b, j], d2d_s.at[b, j], d2d_r.at[b, j], to_core
        )

    def x_copy(b, j, n):
        a = acc.at[b, j]
        src, dst, peer = (
            (a.at[x2], r1.at[b, j, 0], to_xp),
            (a.at[4 + x2], r1.at[b, j, 1], to_xm),
            (a.at[4 + xp], fin.at[b, j, 0, 1], to_xp),
            (a.at[xm], fin.at[b, j, 1, 0], to_xm),
            (a.at[xp], fin.at[b, j, 0, 0], to_xp),
            (a.at[4 + xm], fin.at[b, j, 1, 1], to_xm),
        )[n]
        return send(src, dst, x_s.at[b, j, n], x_r.at[b, j, n], peer)

    def y_copy(b, j):
        return send(xs.at[b, j, 1 - yh], yr.at[b, j], y_s.at[b, j], y_r.at[b, j], to_y)

    def z_copy(b, zt):
        peer = {"tensor": zt * 2 + c}
        return send(zs.at[b, zt], zr.at[b, z], z_s.at[b, zt], z_r.at[b, z], peer)

    def z_recv(b, zt):
        peer = {"tensor": zt * 2 + c}
        return send(zs.at[b, zt], zr.at[b, zt], z_s.at[b, zt], z_r.at[b, zt], peer)

    def c_copy(zt):
        return send(cs, cr.at[z], c_s.at[zt], c_r.at[z], {"tensor": zt * 2 + c})

    def c_recv(zt):
        return send(cs, cr.at[zt], c_s.at[zt], c_r.at[zt], {"tensor": zt * 2 + c})

    def h_copy(t):
        return send(hs.at[t % 2], hg.at[tensor], h_s.at[t], h_r.at[tensor], {"tensor": t})

    def h_recv(t):
        return send(hs.at[t % 2], hg.at[t], h_s.at[t], h_r.at[t], {"tensor": t})

    def each(n, f):
        def body(i, _):
            f(i)
            return 0

        lax.fori_loop(0, n, body, 0)

    def project(b, j):
        at = pl.ds(pl.multiple_of(j * CW, CW), CW)
        p = dot(kg[...], wks[at, :], NT) + dot(vg[...], wvs[at, :], NT)
        part[b, j] = p.reshape(8, 2, 32, CW)
        d2d_copy(b, j).start()

    def stage1(b, j):
        d2d_copy(b, j).wait_recv()
        acc[b, j] = part[b, j, :, c] + d2dr[b, j]
        for n in range(4):
            x_copy(b, j, n).start()

    def stage2(b, j):
        x_copy(b, j, 0).wait_recv()
        acc[b, j, xp] = acc[b, j, xp] + r1[b, j, 0]
        x_copy(b, j, 4).start()
        x_copy(b, j, 1).wait_recv()
        acc[b, j, 4 + xm] = acc[b, j, 4 + xm] + r1[b, j, 1]
        x_copy(b, j, 5).start()

    def stage3(b, j):
        for n in range(2, 6):
            x_copy(b, j, n).wait_recv()
        for h in range(2):
            xs[b, j, h] = acc[b, j, h * 4 + x] + fin[b, j, 0, h] + fin[b, j, 1, h]
        y_copy(b, j).start()

    def stage4(b, j):
        y_copy(b, j).wait_recv()
        total = xs[b, j, yh] + yr[b, j]
        for n in range(CW // 128):
            zt = j * (CW // 128) + n
            block = total[:, n * 128 : (n + 1) * 128]
            zs[b, zt] = block
            crossp[pl.ds(b * 32, 32), :] += block * gh[b, zt]

            @pl.when(zt != z)
            def _():
                z_copy(b, zt).start()

    def head(i):
        for copy in loads(i):
            copy.wait()
        cols = pl.ds(pl.multiple_of((i % HEADS) * DK, DK), DK)
        scores = dot(ks[i], qs[i], NT)
        top = jnp.max(scores, axis=0, keepdims=True)
        shifted = jnp.exp(scores - top)
        probs = shifted * (1.0 / jnp.sum(shifted, axis=0, keepdims=True))
        probs_low = probs.astype(BF16)
        prob_grad = dot(vs[i], gs[i], NT)
        row_dot = jnp.sum(probs_low.astype(F32) * prob_grad, axis=0, keepdims=True)
        score_low = (probs * (prob_grad - row_dot)).astype(BF16)
        vg[:, cols] = dot(probs_low, gs[i], NN).astype(BF16)
        kg[:, cols] = dot(score_low, qs[i], NN).astype(BF16)

    def gather_hidden():
        gain8 = jnp.broadcast_to(gain_ref[...], (8, 64))
        for half in range(2):
            for b in range(NSEQ):
                hs[half, b * 32 : (b + 1) * 32] = hid_ref[b, half * 32 : (half + 1) * 32]
            hs[half, 64:72] = gain8

        def start(d):
            h_copy((tensor + d + 1) % 16).start()

        each(15, start)
        hg[tensor] = hs[c]

    def take_hidden():
        def wait(d):
            h_recv((tensor + d + 1) % 16).wait_recv()

        each(15, wait)
        for zt in range(8):
            both = jnp.concatenate([hg[2 * zt], hg[2 * zt + 1]], axis=-1)
            for b in range(NSEQ):
                gh[b, zt] = both[b * 32 : (b + 1) * 32] * both[64:65]
        crossp[...] = jnp.zeros_like(crossp)

    def step(i, _):
        @pl.when(i == HEADS)
        def _():
            pl.semaphore_wait(barrier, 18)
            gather_hidden()
            for copy in wcopies:
                copy.wait()
            each(NJ, lambda j: project(0, j))

        head(i)

        @pl.when(i == HEADS)
        def _():
            each(NJ, lambda j: stage1(0, j))

        @pl.when(i == HEADS + 3)
        def _():
            each(NJ, lambda j: stage2(0, j))

        @pl.when(i == HEADS + 6)
        def _():
            take_hidden()
            each(NJ, lambda j: stage3(0, j))

        return 0

    lax.fori_loop(0, NSEQ * HEADS, step, 0)

    for j in range(NJ):
        project(1, j)
        if j > 0:
            stage1(1, j - 1)
    stage1(1, NJ - 1)
    each(NJ, lambda j: stage4(0, j))
    for j in range(NJ):
        stage2(1, j)
    for j in range(NJ):
        stage3(1, j)
        if j > 0:
            stage4(1, j - 1)
    stage4(1, NJ - 1)

    cs[...] = dot(jnp.ones((8, 128), F32), crossp[...], NT, precision=lax.Precision.HIGHEST)

    def start_cross(d):
        c_copy((z + d + 1) % 8).start()

    each(7, start_cross)

    mine = jnp.concatenate([hg[2 * z], hg[2 * z + 1]], axis=-1)
    square = jnp.zeros((64, 64), F32)
    for t in range(16):
        part_of = hg[t, :64]
        square = square + part_of * part_of
    square = jnp.sum(square, axis=-1, keepdims=True)
    inverse = lax.rsqrt(square * (1.0 / D) + EPS)

    def wait_z(d):
        zt = (z + d + 1) % 8
        z_recv(0, zt).wait_recv()
        z_recv(1, zt).wait_recv()
        c_recv(zt).wait_recv()

    each(7, wait_z)
    zr[0, z] = zs[0, z]
    zr[1, z] = zs[1, z]
    cr[z] = cs[...]
    cross = cr[0]
    for t in range(1, 8):
        cross = cross + cr[t]
    wide = jnp.broadcast_to(cross[:1], (64, 128))
    row = lax.broadcasted_iota(jnp.int32, (64, 128), 0)
    lane = lax.broadcasted_iota(jnp.int32, (64, 128), 1)
    cross_col = jnp.sum(jnp.where(row == lane, wide, 0.0), axis=-1, keepdims=True)
    gain_mine, hid_mine = mine[64:65], mine[:64]
    scale = cross_col * inverse * inverse * inverse * (1.0 / D)
    for b in range(NSEQ):
        rows = slice(b * 32, (b + 1) * 32)
        grad = zr[b, 0]
        for t in range(1, 8):
            grad = grad + zr[b, t]
        done = gain_mine * grad * inverse[rows] - hid_mine[rows] * scale[rows]
        own = jnp.where(c == 0, done[:, :64], done[:, 64:])
        osend[b] = jnp.where(c == 0, done[:, 64:], done[:, :64])
        out_ref[b, pl.ds(pl.multiple_of(c * 32, 32), 32), :] = own
    o_copy = send(osend, orecv, o_s, o_r, to_core)
    o_copy.start()

    def sends(n):
        b, j = n // NJ, n % NJ
        d2d_copy(b, j).wait_send()
        y_copy(b, j).wait_send()
        for k in range(6):
            x_copy(b, j, k).wait_send()

    each(NSEQ * NJ, sends)

    def small_sends(d):
        zt = (z + d + 1) % 8
        z_copy(0, zt).wait_send()
        z_copy(1, zt).wait_send()
        c_copy(zt).wait_send()

    each(7, small_sends)
    each(15, lambda d: h_copy((tensor + d + 1) % 16).wait_send())
    o_copy.wait()
    for b in range(NSEQ):
        out_ref[b, pl.ds(pl.multiple_of((1 - c) * 32, 32), 32), :] = orecv[b]


def per_device(q, k, v, g, wk, wv, hidden, gain):
    dma = pltpu.SemaphoreType.DMA
    vm = pltpu.VMEM
    anywhere = pl.BlockSpec(memory_space=pl.ANY)
    vmem = pl.BlockSpec(memory_space=pltpu.VMEM)
    heads = vm((NSEQ * HEADS, ROWS, DK), BF16)
    return pl.pallas_call(
        kernel,
        out_shape=jax.ShapeDtypeStruct((NSEQ, 64, 64), F32),
        in_specs=[anywhere] * 6 + [vmem] * 2,
        out_specs=vmem,
        scratch_shapes=[
            heads, heads, heads, heads,
            vm((D, D), BF16), vm((D, D), BF16),
            vm((ROWS, D), BF16), vm((ROWS, D), BF16),
            vm((NSEQ, NJ, 8, 2, 32, CW), F32),
            vm((NSEQ, NJ, 8, 32, CW), F32),
            vm((NSEQ, NJ, 8, 32, CW), F32),
            vm((NSEQ, NJ, 2, 32, CW), F32),
            vm((NSEQ, NJ, 2, 2, 32, CW), F32),
            vm((NSEQ, NJ, 2, 32, CW), F32),
            vm((NSEQ, NJ, 32, CW), F32),
            vm((NSEQ, 8, 32, 128), F32),
            vm((NSEQ, 8, 32, 128), F32),
            vm((8, 128), F32),
            vm((8, 8, 128), F32),
            vm((2, 72, 64), F32),
            vm((16, 72, 64), F32),
            vm((NSEQ, 8, 32, 128), F32),
            vm((128, 128), F32),
            vm((NSEQ, 32, 64), F32),
            vm((NSEQ, 32, 64), F32),
            dma((NSEQ * HEADS, 4)), dma((2,)),
            dma((NSEQ, NJ)), dma((NSEQ, NJ)),
            dma((NSEQ, NJ, 6)), dma((NSEQ, NJ, 6)),
            dma((NSEQ, NJ)), dma((NSEQ, NJ)),
            dma((NSEQ, 8)), dma((NSEQ, 8)),
            dma((8,)), dma((8,)),
            dma((16,)), dma((16,)),
            dma, dma,
        ],
        compiler_params=pltpu.CompilerParams(
            collective_id=0, has_side_effects=True, vmem_limit_bytes=56 * 1024 * 1024
        ),
    )(q, k, v, g, wk, wv, hidden, gain.reshape(1, 64))


def solution(mesh):
    return jax.shard_map(
        per_device,
        mesh=mesh,
        in_specs=(
            P("section", "dp", None, "tensor"),
            P("section", "dp", None, "tensor"),
            P("section", "dp", None, "tensor"),
            P("section", "dp", None, "tensor"),
            P("section", None, "tensor"),
            P("section", None, "tensor"),
            P("dp", "section", "tensor"),
            P("tensor"),
        ),
        out_specs=P("dp", "section", "tensor"),
        check_vma=False,
    )
```

```python
import functools

import jax
import jax.numpy as jnp
from jax import lax
from jax.experimental import pallas as pl
from jax.experimental.pallas import tpu as pltpu
from jax.sharding import PartitionSpec as P

D = 1024
DK = 128
EPS = 1e-06
F32 = jnp.float32
BF16 = jnp.bfloat16
MESH = pl.DeviceIdType.MESH

NSEQ = 2
HEADS = 8
ROWS = 512
NJ = 4
CW = D // NJ
NT = (((1,), (1,)), ((), ()))
NN = (((1,), (0,)), ((), ()))


def dot(a, b, dims, **kw):
    return lax.dot_general(a, b, dims, preferred_element_type=F32, **kw)


def kernel(
    q_hbm, k_hbm, v_hbm, g_hbm, wk_hbm, wv_hbm, hid_ref, gain_ref, out_hbm,
    kqvg, wks, wvs, kg, vg,
    part, d2dr, acc, r1, fin, zs, zr, cs, cr, hs, hp, hg, gh, crossp, oown, osend,
    in_sem, w_sem, d2d_s, d2d_r, x_s, r1_r, fin_r, z_s, z_r, c_s, c_r,
    p_s, p_r, hy_s, hy_r, h_s, h_r, o_l, o_s, o_r,
):
    section = lax.axis_index("section")
    tensor = lax.axis_index("tensor")
    yh, x = section // 4, section % 4
    z, c = tensor // 2, tensor % 2
    xp, xm, x2 = (x + 1) % 4, (x + 3) % 4, (x + 2) % 4
    me = yh * 8 + z
    to_core = {"tensor": z * 2 + (1 - c)}
    to_xp = {"section": yh * 4 + xp}
    to_xm = {"section": yh * 4 + xm}
    to_y = {"section": (1 - yh) * 4 + x}

    def to_yz(n):
        return {"section": n // 8 * 4 + x, "tensor": n % 8 * 2 + c}

    def each(n, f, start=0):
        def body(i, _):
            f(i)
            return 0

        lax.fori_loop(start, n, body, 0)

    def wait_bytes(ref, sem):
        pltpu.make_async_copy(ref, ref, sem).wait()

    def load(i):
        b, h = i // HEADS, i % HEADS
        cols = pl.ds(pl.multiple_of(h * DK, DK), DK)
        for n, src in enumerate((k_hbm, q_hbm, v_hbm, g_hbm)):
            pltpu.make_async_copy(src.at[0, b, :, cols], kqvg.at[i, n], in_sem.at[i]).start()

    wcopies = [
        pltpu.make_async_copy(wk_hbm.at[0], wks, w_sem.at[0]),
        pltpu.make_async_copy(wv_hbm.at[0], wvs, w_sem.at[1]),
    ]
    each(HEADS, load)
    for copy in wcopies:
        copy.start()
    each(NSEQ * HEADS, load, HEADS)

    barrier = pltpu.get_barrier_semaphore()
    for peer in (to_core, to_xp, to_xm):
        pl.semaphore_signal(barrier, inc=1, device_id=peer, device_id_type=MESH)

    def greet(d):
        peer = to_yz((me + d) % 16)
        pl.semaphore_signal(barrier, inc=1, device_id=peer, device_id_type=MESH)

    each(16, greet, 1)

    def send(src, dst, s, r, peer):
        return pltpu.make_async_remote_copy(
            src_ref=src, dst_ref=dst, send_sem=s, recv_sem=r, device_id=peer, device_id_type=MESH
        )

    def x_copy(b, j, n):
        a = acc.at[b, j]
        src, dst, r, peer = (
            (a.at[x2], r1.at[b, j, 0], r1_r.at[b, j, 0], to_xp),
            (a.at[4 + x2], r1.at[b, j, 1], r1_r.at[b, j, 1], to_xm),
            (a.at[4 + xp], fin.at[b, j, 0, 1], fin_r.at[b, j], to_xp),
            (a.at[xm], fin.at[b, j, 1, 0], fin_r.at[b, j], to_xm),
            (a.at[xp], fin.at[b, j, 0, 0], fin_r.at[b, j], to_xp),
            (a.at[4 + xm], fin.at[b, j, 1, 1], fin_r.at[b, j], to_xm),
        )[n]
        return send(src, dst, x_s, r, peer)

    def project(b, j):
        at = pl.ds(pl.multiple_of(j * CW, CW), CW)
        p = dot(kg[...], wks[at, :], NT) + dot(vg[...], wvs[at, :], NT)
        part[b, j] = p.reshape(8, 2, 32, CW)
        send(part.at[b, j, :, 1 - c], d2dr.at[b, j], d2d_s, d2d_r.at[b, j], to_core).start()

    def stage1(b, j):
        wait_bytes(d2dr.at[b, j], d2d_r.at[b, j])
        acc[b, j] = part[b, j, :, c] + d2dr[b, j]
        for n in range(2):
            x_copy(b, j, n).start()

    def stage1b(b, j):
        for n in range(2, 4):
            x_copy(b, j, n).start()

    def stage2(b, j):
        wait_bytes(r1.at[b, j, 0], r1_r.at[b, j, 0])
        acc[b, j, xp] = acc[b, j, xp] + r1[b, j, 0]
        x_copy(b, j, 4).start()
        wait_bytes(r1.at[b, j, 1], r1_r.at[b, j, 1])
        acc[b, j, 4 + xm] = acc[b, j, 4 + xm] + r1[b, j, 1]
        x_copy(b, j, 5).start()

    def stage3(b, j):
        wait_bytes(fin.at[b, j], fin_r.at[b, j])
        for k in range(2):
            h = (1 - yh) if k == 0 else yh
            total = acc[b, j, h * 4 + x] + fin[b, j, 0, h] + fin[b, j, 1, h]
            for n in range(CW // 128):
                zt = j * (CW // 128) + n
                to = h * 8 + zt
                block = total[:, n * 128 : (n + 1) * 128]
                zs[b, to] = block
                crossp[h, pl.ds(pl.multiple_of(b * 32, 32), 32), :] += block * gh[b, h, zt]

                @pl.when(to != me)
                def _():
                    send(zs.at[b, to], zr.at[b, me], z_s, z_r, to_yz(to)).start()

    def head(i):
        wait_bytes(kqvg.at[i], in_sem.at[i])
        cols = pl.ds(pl.multiple_of((i % HEADS) * DK, DK), DK)
        scores = dot(kqvg[i, 0], kqvg[i, 1], NT)
        top = jnp.max(scores, axis=0, keepdims=True)
        shifted = jnp.exp(scores - top)
        probs = shifted * (1.0 / jnp.sum(shifted, axis=0, keepdims=True))
        probs_low = probs.astype(BF16)
        prob_grad = dot(kqvg[i, 2], kqvg[i, 3], NT)
        row_dot = jnp.sum(probs_low.astype(F32) * prob_grad, axis=0, keepdims=True)
        score_low = (probs * (prob_grad - row_dot)).astype(BF16)
        vg[:, cols] = dot(probs_low, kqvg[i, 3], NN).astype(BF16)
        kg[:, cols] = dot(score_low, kqvg[i, 1], NN).astype(BF16)

    def swap_hidden():
        gain8 = jnp.broadcast_to(gain_ref[...], (8, 64))
        for half in range(2):
            for b in range(NSEQ):
                hs[half, b * 32 : (b + 1) * 32] = hid_ref[b, half * 32 : (half + 1) * 32]
            hs[half, 64:72] = gain8
        send(hs.at[1 - c], hp, p_s, p_r, to_core).start()

    def y_rows():
        return hg.at[z, pl.ds(pl.multiple_of(yh * 64, 64), 64)]

    def swap_hidden_y():
        wait_bytes(hp, p_r)
        own, other = hs[c], hp[...]
        both = jnp.where(
            c == 0,
            jnp.concatenate([own, other], axis=-1),
            jnp.concatenate([other, own], axis=-1),
        )
        hg[z, pl.ds(pl.multiple_of(yh * 64, 64), 64), :] = both[:64]
        hg[z, 128:136] = both[64:]
        send(y_rows(), y_rows(), hy_s, hy_r, to_y).start()

    def gather_hidden():
        wait_bytes(y_rows(), hy_r)

        def start(d):
            zt = (z + d) % 8
            send(hg.at[z], hg.at[z], h_s, h_r, {"tensor": zt * 2 + c}).start()

        each(8, start, 1)

    def take_hidden():
        wait_bytes(hg.at[pl.ds(0, 7)], h_r)
        for zt in range(8):
            for h in range(2):
                for b in range(NSEQ):
                    at = h * 64 + b * 32
                    gh[b, h, zt] = hg[zt, at : at + 32] * hg[zt, 128:129]
        crossp[...] = jnp.zeros_like(crossp)

    def step(i, _):
        @pl.when(i == 3)
        def _():
            pl.semaphore_wait(barrier, 18)
            swap_hidden()

        @pl.when(i == 5)
        def _():
            swap_hidden_y()

        @pl.when(i == 7)
        def _():
            gather_hidden()

        @pl.when(i == HEADS)
        def _():
            for copy in wcopies:
                copy.wait()
            each(NJ, lambda j: project(0, j))

        head(i)

        @pl.when(i == HEADS)
        def _():
            each(NJ, lambda j: stage1(0, j))
            each(NJ, lambda j: stage1b(0, j))

        @pl.when(i == HEADS + 4)
        def _():
            each(NJ, lambda j: stage2(0, j))

        @pl.when(i == HEADS + 7)
        def _():
            take_hidden()
            each(NJ, lambda j: stage3(0, j))

        return 0

    lax.fori_loop(0, NSEQ * HEADS, step, 0)

    def tail(t):
        @pl.when(t < NJ)
        def _():
            project(1, t)

        @pl.when((t >= 2) & (t < NJ + 2))
        def _():
            stage1(1, t - 2)
            stage1b(1, t - 2)

        @pl.when((t >= 3) & (t < NJ + 3))
        def _():
            stage2(1, t - 3)

        @pl.when(t >= 5)
        def _():
            stage3(1, t - 5)

    each(NJ + 5, tail)

    for h in range(2):
        cs[h] = dot(jnp.ones((8, 128), F32), crossp[h], NT, precision=lax.Precision.HIGHEST)

    def start_cross(d):
        to = (me + d) % 16
        send(cs.at[to // 8], cr.at[me], c_s, c_r, to_yz(to)).start()

    each(16, start_cross, 1)

    rows = pl.ds(pl.multiple_of(yh * 64, 64), 64)
    hid_mine, gain_mine = hg[z, rows, :], hg[z, 128:129]
    square = jnp.zeros((64, 128), F32)
    for zt in range(8):
        hidden = hg[zt, rows, :]
        square = square + hidden * hidden
    square = jnp.sum(square, axis=-1, keepdims=True)
    inverse = lax.rsqrt(square * (1.0 / D) + EPS)

    def finish():
        wait_bytes(zr.at[:, pl.ds(0, 15)], z_r)
        wait_bytes(cr.at[pl.ds(0, 15)], c_r)

    finish()
    for b in range(NSEQ):
        zr[b, me] = zs[b, me]
    cr[me] = cs[yh]
    cross = cr[0]
    for t in range(1, 16):
        cross = cross + cr[t]
    wide = jnp.broadcast_to(cross[:1], (64, 128))
    row = lax.broadcasted_iota(jnp.int32, (64, 128), 0)
    lane = lax.broadcasted_iota(jnp.int32, (64, 128), 1)
    cross_col = jnp.sum(jnp.where(row == lane, wide, 0.0), axis=-1, keepdims=True)
    scale = cross_col * inverse * inverse * inverse * (1.0 / D)
    for b in range(NSEQ):
        at = slice(b * 32, (b + 1) * 32)
        grad = zr[b, 0]
        for t in range(1, 16):
            grad = grad + zr[b, t]
        done = gain_mine * grad * inverse[at] - hid_mine[at] * scale[at]
        oown[b] = jnp.where(c == 0, done[:, :64], done[:, 64:])
        osend[b] = jnp.where(c == 0, done[:, 64:], done[:, :64])
    half = out_hbm.at[:, pl.ds(pl.multiple_of(c * 32, 32), 32), :]
    other = out_hbm.at[:, pl.ds(pl.multiple_of((1 - c) * 32, 32), 32), :]
    away = send(osend, half, o_s, o_r, to_core)
    away.start()
    here = pltpu.make_async_copy(oown, half, o_l)
    here.start()

    wait_bytes(d2dr, d2d_s)
    wait_bytes(acc.at[:, :, pl.ds(0, 6)], x_s)
    wait_bytes(zs.at[:, pl.ds(0, 15)], z_s)
    wait_bytes(cr.at[pl.ds(0, 15)], c_s)
    wait_bytes(hp, p_s)
    wait_bytes(y_rows(), hy_s)
    wait_bytes(hg.at[pl.ds(0, 7)], h_s)
    here.wait()
    away.wait_send()
    wait_bytes(other, o_r)


def per_device(q, k, v, g, wk, wv, hidden, gain):
    dma = pltpu.SemaphoreType.DMA
    vm = pltpu.VMEM
    anywhere = pl.BlockSpec(memory_space=pl.ANY)
    vmem = pl.BlockSpec(memory_space=pltpu.VMEM)
    return pl.pallas_call(
        kernel,
        out_shape=jax.ShapeDtypeStruct((NSEQ, 64, 64), F32),
        in_specs=[anywhere] * 6 + [vmem] * 2,
        out_specs=anywhere,
        scratch_shapes=[
            vm((NSEQ * HEADS, 4, ROWS, DK), BF16),
            vm((D, D), BF16), vm((D, D), BF16),
            vm((ROWS, D), BF16), vm((ROWS, D), BF16),
            vm((NSEQ, NJ, 8, 2, 32, CW), F32),
            vm((NSEQ, NJ, 8, 32, CW), F32),
            vm((NSEQ, NJ, 8, 32, CW), F32),
            vm((NSEQ, NJ, 2, 32, CW), F32),
            vm((NSEQ, NJ, 2, 2, 32, CW), F32),
            vm((NSEQ, 16, 32, 128), F32),
            vm((NSEQ, 16, 32, 128), F32),
            vm((2, 8, 128), F32),
            vm((16, 8, 128), F32),
            vm((2, 72, 64), F32),
            vm((72, 64), F32),
            vm((8, 136, 128), F32),
            vm((NSEQ, 2, 8, 32, 128), F32),
            vm((2, 128, 128), F32),
            vm((NSEQ, 32, 64), F32),
            vm((NSEQ, 32, 64), F32),
            dma((NSEQ * HEADS,)), dma((2,)),
            dma, dma((NSEQ, NJ)),
            dma, dma((NSEQ, NJ, 2)), dma((NSEQ, NJ)),
            dma, dma,
            dma, dma,
            dma, dma, dma, dma, dma, dma,
            dma, dma, dma,
        ],
        compiler_params=pltpu.CompilerParams(
            collective_id=0, has_side_effects=True, vmem_limit_bytes=56 * 1024 * 1024
        ),
    )(q, k, v, g, wk, wv, hidden, gain.reshape(1, 64))


def solution(mesh):
    return jax.shard_map(
        per_device,
        mesh=mesh,
        in_specs=(
            P("section", "dp", None, "tensor"),
            P("section", "dp", None, "tensor"),
            P("section", "dp", None, "tensor"),
            P("section", "dp", None, "tensor"),
            P("section", None, "tensor"),
            P("section", None, "tensor"),
            P("dp", "section", "tensor"),
            P("tensor"),
        ),
        out_specs=P("dp", "section", "tensor"),
        check_vma=False,
    )
```

```python
import functools

import jax
import jax.numpy as jnp
from jax import lax
from jax.experimental import pallas as pl
from jax.experimental.pallas import tpu as pltpu
from jax.sharding import PartitionSpec as P

D = 1024
DK = 128
EPS = 1e-06
F32 = jnp.float32
BF16 = jnp.bfloat16
MESH = pl.DeviceIdType.MESH

NSEQ = 2
HEADS = 8
ROWS = 512
GROUP = 4
NJ = 4
CW = D // NJ
NT = (((1,), (1,)), ((), ()))
NN = (((1,), (0,)), ((), ()))


def dot(a, b, dims, **kw):
    return lax.dot_general(a, b, dims, preferred_element_type=F32, **kw)


def kernel(
    q_hbm, k_hbm, v_hbm, g_hbm, wk_hbm, wv_hbm, hid_ref, gain_ref, out_hbm,
    kqvg, wks, wvs, kg, vg,
    part, d2dr, acc, r1, fin, zs, zr, cs, cr, hs, hr, hg, gh, crossp, oown, osend,
    in_sem, w_sem, d2d_s, d2d_r, x_s, r1_r, fin_r, z_s, z_r, c_s, c_r,
    h_s, h_r, o_l, o_s, o_r,
):
    section = lax.axis_index("section")
    tensor = lax.axis_index("tensor")
    yh, x = section // 4, section % 4
    z, c = tensor // 2, tensor % 2
    xp, xm, x2 = (x + 1) % 4, (x + 3) % 4, (x + 2) % 4
    me = yh * 8 + z
    me32 = yh * 16 + tensor
    to_core = {"tensor": z * 2 + (1 - c)}
    to_xp = {"section": yh * 4 + xp}
    to_xm = {"section": yh * 4 + xm}
    to_y = {"section": (1 - yh) * 4 + x}

    def to_yz(n):
        return {"section": n // 8 * 4 + x, "tensor": n % 8 * 2 + c}

    def each(n, f, start=0):
        def body(i, _):
            f(i)
            return 0

        lax.fori_loop(start, n, body, 0)

    def wait_bytes(ref, sem):
        pltpu.make_async_copy(ref, ref, sem).wait()

    def load(i):
        b, h = i // HEADS, i % HEADS
        cols = pl.ds(pl.multiple_of(h * DK, DK), DK)
        for n, src in enumerate((k_hbm, q_hbm, v_hbm, g_hbm)):
            pltpu.make_async_copy(src.at[0, b, :, cols], kqvg.at[i, n], in_sem.at[i]).start()

    wcopies = [
        pltpu.make_async_copy(wk_hbm.at[0], wks, w_sem.at[0]),
        pltpu.make_async_copy(wv_hbm.at[0], wvs, w_sem.at[1]),
    ]
    each(HEADS, load)

    barrier = pltpu.get_barrier_semaphore()
    for peer in (to_xp, to_xm):
        pl.semaphore_signal(barrier, inc=1, device_id=peer, device_id_type=MESH)

    def greet(d):
        to = (me32 + d) % 32
        peer = {"section": to // 16 * 4 + x, "tensor": to % 16}
        pl.semaphore_signal(barrier, inc=1, device_id=peer, device_id_type=MESH)

    each(32, greet, 1)
    for copy in wcopies:
        copy.start()

    def send(src, dst, s, r, peer):
        return pltpu.make_async_remote_copy(
            src_ref=src, dst_ref=dst, send_sem=s, recv_sem=r, device_id=peer, device_id_type=MESH
        )

    def x_copy(b, j, n):
        a = acc.at[b, j]
        src, dst, r, peer = (
            (a.at[x2], r1.at[b, j, 0], r1_r.at[b, j, 0], to_xp),
            (a.at[4 + x2], r1.at[b, j, 1], r1_r.at[b, j, 1], to_xm),
            (a.at[4 + xp], fin.at[b, j, 0, 1], fin_r.at[b, j], to_xp),
            (a.at[xm], fin.at[b, j, 1, 0], fin_r.at[b, j], to_xm),
            (a.at[xp], fin.at[b, j, 0, 0], fin_r.at[b, j], to_xp),
            (a.at[4 + xm], fin.at[b, j, 1, 1], fin_r.at[b, j], to_xm),
        )[n]
        return send(src, dst, x_s, r, peer)

    def project(b, j):
        at = pl.ds(pl.multiple_of(j * CW, CW), CW)
        p = dot(kg[...], wks[at, :], NT) + dot(vg[...], wvs[at, :], NT)
        part[b, j] = p.reshape(8, 2, 32, CW)
        send(part.at[b, j, :, 1 - c], d2dr.at[b, j], d2d_s, d2d_r.at[b, j], to_core).start()

    def stage1(b, j):
        wait_bytes(d2dr.at[b, j], d2d_r.at[b, j])
        acc[b, j] = part[b, j, :, c] + d2dr[b, j]
        for n in range(2):
            x_copy(b, j, n).start()

    def stage1b(b, j):
        for n in range(2, 4):
            x_copy(b, j, n).start()

    def stage2(b, j):
        wait_bytes(r1.at[b, j, 0], r1_r.at[b, j, 0])
        acc[b, j, xp] = acc[b, j, xp] + r1[b, j, 0]
        x_copy(b, j, 4).start()
        wait_bytes(r1.at[b, j, 1], r1_r.at[b, j, 1])
        acc[b, j, 4 + xm] = acc[b, j, 4 + xm] + r1[b, j, 1]
        x_copy(b, j, 5).start()

    def stage3(b, j):
        wait_bytes(fin.at[b, j], fin_r.at[b, j])
        for k in range(2):
            h = (1 - yh) if k == 0 else yh
            total = acc[b, j, h * 4 + x] + fin[b, j, 0, h] + fin[b, j, 1, h]
            for n in range(CW // 128):
                zt = j * (CW // 128) + n
                to = h * 8 + zt
                block = total[:, n * 128 : (n + 1) * 128]
                zs[b, to] = block
                crossp[h, pl.ds(pl.multiple_of(b * 32, 32), 32), :] += block * gh[b, h, zt]

                @pl.when(to != me)
                def _():
                    send(zs.at[b, to], zr.at[b, me], z_s, z_r, to_yz(to)).start()

    def head(i):
        cols = pl.ds(pl.multiple_of((i % HEADS) * DK, DK), DK)
        scores = dot(kqvg[i, 0], kqvg[i, 1], NT)
        top = jnp.max(scores, axis=0, keepdims=True)
        shifted = jnp.exp(scores - top)
        probs = shifted * (1.0 / jnp.sum(shifted, axis=0, keepdims=True))
        probs_low = probs.astype(BF16)
        prob_grad = dot(kqvg[i, 2], kqvg[i, 3], NT)
        row_dot = jnp.sum(probs_low.astype(F32) * prob_grad, axis=0, keepdims=True)
        score_low = (probs * (prob_grad - row_dot)).astype(BF16)
        vg[:, cols] = dot(probs_low, kqvg[i, 3], NN).astype(BF16)
        kg[:, cols] = dot(score_low, kqvg[i, 1], NN).astype(BF16)

    def gather_hidden():
        gain8 = jnp.broadcast_to(gain_ref[...], (8, 64))
        for half in range(2):
            at = slice(half * 32, (half + 1) * 32)
            hs[half, :32] = jnp.concatenate([hid_ref[0, at], hid_ref[1, at]], axis=-1)
            hs[half, 32:] = jnp.concatenate([gain8, gain8], axis=-1)
        hr[me32] = hs[c]

        def start(d):
            to = (me32 + d) % 32
            peer = {"section": to // 16 * 4 + x, "tensor": to % 16}
            send(hs.at[to % 2], hr.at[me32], h_s, h_r, peer).start()

        each(32, start, 1)

    def take_hidden():
        wait_bytes(hr.at[pl.ds(0, 31)], h_r)
        low = lax.broadcasted_iota(jnp.int32, (40, 128), 1) < 64
        for h in range(2):
            for zt in range(8):
                even, odd = hr[h * 16 + 2 * zt], hr[h * 16 + 2 * zt + 1]
                first = jnp.where(low, even, pltpu.roll(odd, 64, 1))
                second = jnp.where(low, pltpu.roll(even, 64, 1), odd)
                gain_row = first[32:33]
                for b, hidden in enumerate((first[:32], second[:32])):
                    hg[h, zt, b * 32 : (b + 1) * 32] = hidden
                    gh[b, h, zt] = hidden * gain_row
                hg[h, zt, 64:72] = first[32:]
        crossp[...] = jnp.zeros_like(crossp)

    def group(n):
        @pl.when(n == 1)
        def _():
            pl.semaphore_wait(barrier, 33)
            gather_hidden()

        @pl.when(n == HEADS // GROUP)
        def _():
            for copy in wcopies:
                copy.wait()

            def first(t):
                @pl.when(t < NJ)
                def _():
                    project(0, t)

                @pl.when(t >= 2)
                def _():
                    stage1(0, t - 2)

            each(NJ + 2, first)
            each(NJ, lambda j: stage1b(0, j))

        @pl.when(n == HEADS // GROUP + 1)
        def _():
            each(NJ, lambda j: stage2(0, j))

        @pl.when(n < HEADS // GROUP)
        def _():
            each((n + 1) * GROUP + HEADS, load, n * GROUP + HEADS)

        for k in range(GROUP):
            wait_bytes(kqvg.at[n * GROUP + k], in_sem.at[n * GROUP + k])
        for k in range(GROUP):
            head(n * GROUP + k)

    each(NSEQ * HEADS // GROUP, group)
    take_hidden()

    def tail(t):
        @pl.when(t < NJ)
        def _():
            project(1, t)
            stage3(0, t)

        @pl.when((t >= 2) & (t < NJ + 2))
        def _():
            stage1(1, t - 2)
            stage1b(1, t - 2)

        @pl.when((t >= 3) & (t < NJ + 3))
        def _():
            stage2(1, t - 3)

        @pl.when(t >= 5)
        def _():
            stage3(1, t - 5)

    each(NJ + 5, tail)

    for h in range(2):
        cs[h] = dot(jnp.ones((8, 128), F32), crossp[h], NT, precision=lax.Precision.HIGHEST)

    def start_cross(d):
        to = (me + d) % 16
        send(cs.at[to // 8], cr.at[me], c_s, c_r, to_yz(to)).start()

    each(16, start_cross, 1)

    hid_mine, gain_mine = hg[yh, z, :64], hg[yh, z, 64:65]
    square = jnp.zeros((64, 128), F32)
    for zt in range(8):
        hidden = hg[yh, zt, :64]
        square = square + hidden * hidden
    square = jnp.sum(square, axis=-1, keepdims=True)
    inverse = lax.rsqrt(square * (1.0 / D) + EPS)

    def finish():
        wait_bytes(zr.at[:, pl.ds(0, 15)], z_r)
        wait_bytes(cr.at[pl.ds(0, 15)], c_r)

    finish()
    for b in range(NSEQ):
        zr[b, me] = zs[b, me]
    cr[me] = cs[yh]
    cross = cr[0]
    for t in range(1, 16):
        cross = cross + cr[t]
    wide = jnp.broadcast_to(cross[:1], (64, 128))
    row = lax.broadcasted_iota(jnp.int32, (64, 128), 0)
    lane = lax.broadcasted_iota(jnp.int32, (64, 128), 1)
    cross_col = jnp.sum(jnp.where(row == lane, wide, 0.0), axis=-1, keepdims=True)
    scale = cross_col * inverse * inverse * inverse * (1.0 / D)
    for b in range(NSEQ):
        at = slice(b * 32, (b + 1) * 32)
        grad = zr[b, 0]
        for t in range(1, 16):
            grad = grad + zr[b, t]
        done = gain_mine * grad * inverse[at] - hid_mine[at] * scale[at]
        oown[b] = jnp.where(c == 0, done[:, :64], done[:, 64:])
        osend[b] = jnp.where(c == 0, done[:, 64:], done[:, :64])
    half = out_hbm.at[:, pl.ds(pl.multiple_of(c * 32, 32), 32), :]
    other = out_hbm.at[:, pl.ds(pl.multiple_of((1 - c) * 32, 32), 32), :]
    away = send(osend, half, o_s, o_r, to_core)
    away.start()
    here = pltpu.make_async_copy(oown, half, o_l)
    here.start()

    wait_bytes(d2dr, d2d_s)
    wait_bytes(acc.at[:, :, pl.ds(0, 6)], x_s)
    wait_bytes(zs.at[:, pl.ds(0, 15)], z_s)
    wait_bytes(cr.at[pl.ds(0, 15)], c_s)
    wait_bytes(hr.at[pl.ds(0, 31)], h_s)
    here.wait()
    away.wait_send()
    wait_bytes(other, o_r)


def per_device(q, k, v, g, wk, wv, hidden, gain):
    dma = pltpu.SemaphoreType.DMA
    vm = pltpu.VMEM
    anywhere = pl.BlockSpec(memory_space=pl.ANY)
    vmem = pl.BlockSpec(memory_space=pltpu.VMEM)
    return pl.pallas_call(
        kernel,
        out_shape=jax.ShapeDtypeStruct((NSEQ, 64, 64), F32),
        in_specs=[anywhere] * 6 + [vmem] * 2,
        out_specs=anywhere,
        scratch_shapes=[
            vm((NSEQ * HEADS, 4, ROWS, DK), BF16),
            vm((D, D), BF16), vm((D, D), BF16),
            vm((ROWS, D), BF16), vm((ROWS, D), BF16),
            vm((NSEQ, NJ, 8, 2, 32, CW), F32),
            vm((NSEQ, NJ, 8, 32, CW), F32),
            vm((NSEQ, NJ, 8, 32, CW), F32),
            vm((NSEQ, NJ, 2, 32, CW), F32),
            vm((NSEQ, NJ, 2, 2, 32, CW), F32),
            vm((NSEQ, 16, 32, 128), F32),
            vm((NSEQ, 16, 32, 128), F32),
            vm((2, 8, 128), F32),
            vm((16, 8, 128), F32),
            vm((2, 40, 128), F32),
            vm((32, 40, 128), F32),
            vm((2, 8, 72, 128), F32),
            vm((NSEQ, 2, 8, 32, 128), F32),
            vm((2, 128, 128), F32),
            vm((NSEQ, 32, 64), F32),
            vm((NSEQ, 32, 64), F32),
            dma((NSEQ * HEADS,)), dma((2,)),
            dma, dma((NSEQ, NJ)),
            dma, dma((NSEQ, NJ, 2)), dma((NSEQ, NJ)),
            dma, dma,
            dma, dma,
            dma, dma,
            dma, dma, dma,
        ],
        compiler_params=pltpu.CompilerParams(
            collective_id=0, has_side_effects=True, vmem_limit_bytes=56 * 1024 * 1024
        ),
    )(q, k, v, g, wk, wv, hidden, gain.reshape(1, 64))


def solution(mesh):
    return jax.shard_map(
        per_device,
        mesh=mesh,
        in_specs=(
            P("section", "dp", None, "tensor"),
            P("section", "dp", None, "tensor"),
            P("section", "dp", None, "tensor"),
            P("section", "dp", None, "tensor"),
            P("section", None, "tensor"),
            P("section", None, "tensor"),
            P("dp", "section", "tensor"),
            P("tensor"),
        ),
        out_specs=P("dp", "section", "tensor"),
        check_vma=False,
    )
```

```python
import functools

import jax
import jax.numpy as jnp
from jax import lax
from jax.experimental import pallas as pl
from jax.experimental.pallas import tpu as pltpu
from jax.sharding import PartitionSpec as P

D = 1024
DK = 128
EPS = 1e-06
F32 = jnp.float32
BF16 = jnp.bfloat16
MESH = pl.DeviceIdType.MESH

NSEQ = 2
HEADS = 8
ROWS = 512
GROUP = 4
NJ = 4
CW = D // NJ
NT = (((1,), (1,)), ((), ()))
NN = (((1,), (0,)), ((), ()))


def dot(a, b, dims, **kw):
    return lax.dot_general(a, b, dims, preferred_element_type=F32, **kw)


def kernel(
    q_hbm, k_hbm, v_hbm, g_hbm, wk_hbm, wv_hbm, hid_ref, gain_ref, out_hbm,
    kqvg, wks, wvs, kg, vg,
    part, d2dr, acc, r1, fin, zs, zr, cs, cr, hs, hr, hg, gh, crossp, oown, osend,
    in_sem, w_sem, d2d_s, d2d_r, x_s, r1_r, fin_r, z_s, z_r, c_s, c_r,
    h_s, h_r, o_l, o_s, o_r,
):
    section = lax.axis_index("section")
    tensor = lax.axis_index("tensor")
    yh, x = lax.div(section, 4), lax.rem(section, 4)
    z, c = lax.div(tensor, 2), lax.rem(tensor, 2)
    xp, xm, x2 = lax.rem(x + 1, 4), lax.rem(x + 3, 4), lax.rem(x + 2, 4)
    me = yh * 8 + z
    me32 = yh * 16 + tensor
    to_core = {"tensor": z * 2 + (1 - c)}
    to_xp = {"section": yh * 4 + xp}
    to_xm = {"section": yh * 4 + xm}
    to_y = {"section": (1 - yh) * 4 + x}

    def to_yz(n):
        return {"section": lax.div(n, 8) * 4 + x, "tensor": lax.rem(n, 8) * 2 + c}

    def each(n, f, start=0):
        def body(i, _):
            f(i)
            return 0

        lax.fori_loop(start, n, body, 0)

    def wait_bytes(ref, sem):
        pltpu.make_async_copy(ref, ref, sem).wait()

    def load(i):
        b, h = i // HEADS, i % HEADS
        cols = pl.ds(pl.multiple_of(h * DK, DK), DK)
        for n, src in enumerate((k_hbm, q_hbm, v_hbm, g_hbm)):
            pltpu.make_async_copy(src.at[0, b, :, cols], kqvg.at[i, n], in_sem.at[i]).start()

    wcopies = [
        pltpu.make_async_copy(wk_hbm.at[0], wks, w_sem.at[0]),
        pltpu.make_async_copy(wv_hbm.at[0], wvs, w_sem.at[1]),
    ]
    each(HEADS, load)

    barrier = pltpu.get_barrier_semaphore()
    for peer in (to_xp, to_xm):
        pl.semaphore_signal(barrier, inc=1, device_id=peer, device_id_type=MESH)

    def greet(d):
        to = lax.rem(me32 + d, 32)
        peer = {"section": lax.div(to, 16) * 4 + x, "tensor": lax.rem(to, 16)}
        pl.semaphore_signal(barrier, inc=1, device_id=peer, device_id_type=MESH)

    each(32, greet, 1)
    for copy in wcopies:
        copy.start()

    def send(src, dst, s, r, peer):
        return pltpu.make_async_remote_copy(
            src_ref=src, dst_ref=dst, send_sem=s, recv_sem=r, device_id=peer, device_id_type=MESH
        )

    def x_copy(b, j, n):
        a = acc.at[b, j]
        src, dst, r, peer = (
            (a.at[x2], r1.at[b, j, 0], r1_r.at[b, j, 0], to_xp),
            (a.at[4 + x2], r1.at[b, j, 1], r1_r.at[b, j, 1], to_xm),
            (a.at[4 + xp], fin.at[b, j, 0, 1], fin_r.at[b, j], to_xp),
            (a.at[xm], fin.at[b, j, 1, 0], fin_r.at[b, j], to_xm),
            (a.at[xp], fin.at[b, j, 0, 0], fin_r.at[b, j], to_xp),
            (a.at[4 + xm], fin.at[b, j, 1, 1], fin_r.at[b, j], to_xm),
        )[n]
        return send(src, dst, x_s, r, peer)

    def project(b, j):
        at = pl.ds(pl.multiple_of(j * CW, CW), CW)
        p = dot(kg[...], wks[at, :], NT) + dot(vg[...], wvs[at, :], NT)
        part[b, j] = p.reshape(8, 2, 32, CW)
        send(part.at[b, j, :, 1 - c], d2dr.at[b, j], d2d_s, d2d_r.at[b, j], to_core).start()

    def stage1(b, j):
        wait_bytes(d2dr.at[b, j], d2d_r.at[b, j])
        acc[b, j] = part[b, j, :, c] + d2dr[b, j]
        for n in range(2):
            x_copy(b, j, n).start()

    def stage1b(b, j):
        for n in range(2, 4):
            x_copy(b, j, n).start()

    def stage2(b, j):
        wait_bytes(r1.at[b, j, 0], r1_r.at[b, j, 0])
        acc[b, j, xp] = acc[b, j, xp] + r1[b, j, 0]
        x_copy(b, j, 4).start()
        wait_bytes(r1.at[b, j, 1], r1_r.at[b, j, 1])
        acc[b, j, 4 + xm] = acc[b, j, 4 + xm] + r1[b, j, 1]
        x_copy(b, j, 5).start()

    def stage3(b, j):
        wait_bytes(fin.at[b, j], fin_r.at[b, j])
        for k in range(2):
            h = (1 - yh) if k == 0 else yh
            total = acc[b, j, h * 4 + x] + fin[b, j, 0, h] + fin[b, j, 1, h]
            for n in range(CW // 128):
                zt = j * (CW // 128) + n
                to = h * 8 + zt
                block = total[:, n * 128 : (n + 1) * 128]
                zs[b, to] = block
                crossp[h, pl.ds(pl.multiple_of(b * 32, 32), 32), :] += block * gh[b, h, zt]

                @pl.when(to != me)
                def _():
                    send(zs.at[b, to], zr.at[b, me], z_s, z_r, to_yz(to)).start()

    def head(i):
        cols = pl.ds(pl.multiple_of((i % HEADS) * DK, DK), DK)
        scores = dot(kqvg[i, 0], kqvg[i, 1], NT)
        top = jnp.max(scores, axis=0, keepdims=True)
        shifted = jnp.exp(scores - top)
        probs = shifted * (1.0 / jnp.sum(shifted, axis=0, keepdims=True))
        probs_low = probs.astype(BF16)
        prob_grad = dot(kqvg[i, 2], kqvg[i, 3], NT)
        row_dot = jnp.sum(probs_low.astype(F32) * prob_grad, axis=0, keepdims=True)
        score_low = (probs * (prob_grad - row_dot)).astype(BF16)
        vg[:, cols] = dot(probs_low, kqvg[i, 3], NN).astype(BF16)
        kg[:, cols] = dot(score_low, kqvg[i, 1], NN).astype(BF16)

    def gather_hidden():
        gain8 = jnp.broadcast_to(gain_ref[...], (8, 64))
        for half in range(2):
            at = slice(half * 32, (half + 1) * 32)
            hs[half, :32] = jnp.concatenate([hid_ref[0, at], hid_ref[1, at]], axis=-1)
            hs[half, 32:] = jnp.concatenate([gain8, gain8], axis=-1)
        hr[me32] = hs[c]

        def start(d):
            to = lax.rem(me32 + d, 32)
            peer = {"section": lax.div(to, 16) * 4 + x, "tensor": lax.rem(to, 16)}
            send(hs.at[lax.rem(to, 2)], hr.at[me32], h_s, h_r, peer).start()

        each(32, start, 1)

    def take_hidden():
        wait_bytes(hr.at[pl.ds(0, 31)], h_r)
        low = lax.broadcasted_iota(jnp.int32, (40, 128), 1) < 64
        for h in range(2):
            for zt in range(8):
                even, odd = hr[h * 16 + 2 * zt], hr[h * 16 + 2 * zt + 1]
                first = jnp.where(low, even, pltpu.roll(odd, 64, 1))
                second = jnp.where(low, pltpu.roll(even, 64, 1), odd)
                gain_row = first[32:33]
                for b, hidden in enumerate((first[:32], second[:32])):
                    hg[h, zt, b * 32 : (b + 1) * 32] = hidden
                    gh[b, h, zt] = hidden * gain_row
                hg[h, zt, 64:72] = first[32:]
        crossp[...] = jnp.zeros_like(crossp)

    def group(n):
        @pl.when(n == 1)
        def _():
            pl.semaphore_wait(barrier, 33)
            gather_hidden()

        @pl.when(n == HEADS // GROUP)
        def _():
            for copy in wcopies:
                copy.wait()

            def first(t):
                @pl.when(t < NJ)
                def _():
                    project(0, t)

                @pl.when(t >= 2)
                def _():
                    stage1(0, t - 2)

            each(NJ + 2, first)
            each(NJ, lambda j: stage1b(0, j))

        @pl.when(n == HEADS // GROUP + 1)
        def _():
            each(NJ, lambda j: stage2(0, j))

        @pl.when(n < HEADS // GROUP)
        def _():
            each((n + 1) * GROUP + HEADS, load, n * GROUP + HEADS)

        for k in range(GROUP):
            wait_bytes(kqvg.at[n * GROUP + k], in_sem.at[n * GROUP + k])
        for k in range(GROUP):
            head(n * GROUP + k)

    each(NSEQ * HEADS // GROUP, group)

    def tail(t):
        @pl.when(t < NJ)
        def _():
            project(1, t)

        @pl.when((t >= 2) & (t < NJ + 2))
        def _():
            stage1(1, t - 2)
            stage1b(1, t - 2)

        @pl.when(t == 3)
        def _():
            take_hidden()
            each(NJ, lambda j: stage3(0, j))

        @pl.when((t >= 3) & (t < NJ + 3))
        def _():
            stage2(1, t - 3)

        @pl.when(t >= 5)
        def _():
            stage3(1, t - 5)

    each(NJ + 5, tail)

    for h in range(2):
        cs[h] = dot(jnp.ones((8, 128), F32), crossp[h], NT, precision=lax.Precision.HIGHEST)

    def start_cross(d):
        to = lax.rem(me + d, 16)
        send(cs.at[lax.div(to, 8)], cr.at[me], c_s, c_r, to_yz(to)).start()

    each(16, start_cross, 1)

    hid_mine, gain_mine = hg[yh, z, :64], hg[yh, z, 64:65]
    square = jnp.zeros((64, 128), F32)
    for zt in range(8):
        hidden = hg[yh, zt, :64]
        square = square + hidden * hidden
    square = jnp.sum(square, axis=-1, keepdims=True)
    inverse = lax.rsqrt(square * (1.0 / D) + EPS)

    def finish():
        wait_bytes(zr.at[:, pl.ds(0, 15)], z_r)
        wait_bytes(cr.at[pl.ds(0, 15)], c_r)

    finish()
    for b in range(NSEQ):
        zr[b, me] = zs[b, me]
    cr[me] = cs[yh]
    cross = cr[0]
    for t in range(1, 16):
        cross = cross + cr[t]
    wide = jnp.broadcast_to(cross[:1], (64, 128))
    row = lax.broadcasted_iota(jnp.int32, (64, 128), 0)
    lane = lax.broadcasted_iota(jnp.int32, (64, 128), 1)
    cross_col = jnp.sum(jnp.where(row == lane, wide, 0.0), axis=-1, keepdims=True)
    scale = cross_col * inverse * inverse * inverse * (1.0 / D)
    for b in range(NSEQ):
        at = slice(b * 32, (b + 1) * 32)
        grad = zr[b, 0]
        for t in range(1, 16):
            grad = grad + zr[b, t]
        done = gain_mine * grad * inverse[at] - hid_mine[at] * scale[at]
        oown[b] = jnp.where(c == 0, done[:, :64], done[:, 64:])
        osend[b] = jnp.where(c == 0, done[:, 64:], done[:, :64])
    half = out_hbm.at[:, pl.ds(pl.multiple_of(c * 32, 32), 32), :]
    other = out_hbm.at[:, pl.ds(pl.multiple_of((1 - c) * 32, 32), 32), :]
    away = send(osend, half, o_s, o_r, to_core)
    away.start()
    here = pltpu.make_async_copy(oown, half, o_l)
    here.start()

    wait_bytes(d2dr, d2d_s)
    wait_bytes(acc.at[:, :, pl.ds(0, 6)], x_s)
    wait_bytes(zs.at[:, pl.ds(0, 15)], z_s)
    wait_bytes(cr.at[pl.ds(0, 15)], c_s)
    wait_bytes(hr.at[pl.ds(0, 31)], h_s)
    here.wait()
    away.wait_send()
    wait_bytes(other, o_r)


def per_device(q, k, v, g, wk, wv, hidden, gain):
    dma = pltpu.SemaphoreType.DMA
    vm = pltpu.VMEM
    anywhere = pl.BlockSpec(memory_space=pl.ANY)
    vmem = pl.BlockSpec(memory_space=pltpu.VMEM)
    return pl.pallas_call(
        kernel,
        out_shape=jax.ShapeDtypeStruct((NSEQ, 64, 64), F32),
        in_specs=[anywhere] * 6 + [vmem] * 2,
        out_specs=anywhere,
        scratch_shapes=[
            vm((NSEQ * HEADS, 4, ROWS, DK), BF16),
            vm((D, D), BF16), vm((D, D), BF16),
            vm((ROWS, D), BF16), vm((ROWS, D), BF16),
            vm((NSEQ, NJ, 8, 2, 32, CW), F32),
            vm((NSEQ, NJ, 8, 32, CW), F32),
            vm((NSEQ, NJ, 8, 32, CW), F32),
            vm((NSEQ, NJ, 2, 32, CW), F32),
            vm((NSEQ, NJ, 2, 2, 32, CW), F32),
            vm((NSEQ, 16, 32, 128), F32),
            vm((NSEQ, 16, 32, 128), F32),
            vm((2, 8, 128), F32),
            vm((16, 8, 128), F32),
            vm((2, 40, 128), F32),
            vm((32, 40, 128), F32),
            vm((2, 8, 72, 128), F32),
            vm((NSEQ, 2, 8, 32, 128), F32),
            vm((2, 128, 128), F32),
            vm((NSEQ, 32, 64), F32),
            vm((NSEQ, 32, 64), F32),
            dma((NSEQ * HEADS,)), dma((2,)),
            dma, dma((NSEQ, NJ)),
            dma, dma((NSEQ, NJ, 2)), dma((NSEQ, NJ)),
            dma, dma,
            dma, dma,
            dma, dma,
            dma, dma, dma,
        ],
        compiler_params=pltpu.CompilerParams(
            collective_id=0, has_side_effects=True, vmem_limit_bytes=56 * 1024 * 1024
        ),
    )(q, k, v, g, wk, wv, hidden, gain.reshape(1, 64))


def solution(mesh):
    return jax.shard_map(
        per_device,
        mesh=mesh,
        in_specs=(
            P("section", "dp", None, "tensor"),
            P("section", "dp", None, "tensor"),
            P("section", "dp", None, "tensor"),
            P("section", "dp", None, "tensor"),
            P("section", None, "tensor"),
            P("section", None, "tensor"),
            P("dp", "section", "tensor"),
            P("tensor"),
        ),
        out_specs=P("dp", "section", "tensor"),
        check_vma=False,
    )
```

```python
import functools

import jax
import jax.numpy as jnp
from jax import lax
from jax.experimental import pallas as pl
from jax.experimental.pallas import tpu as pltpu
from jax.sharding import PartitionSpec as P

D = 1024
DK = 128
EPS = 1e-06
F32 = jnp.float32
BF16 = jnp.bfloat16
MESH = pl.DeviceIdType.MESH

NSEQ = 2
HEADS = 8
ROWS = 512
GROUP = 4
NJ = 4
CW = D // NJ
NT = (((1,), (1,)), ((), ()))
NN = (((1,), (0,)), ((), ()))


def dot(a, b, dims, **kw):
    return lax.dot_general(a, b, dims, preferred_element_type=F32, **kw)


def kernel(
    q_hbm, k_hbm, v_hbm, g_hbm, wk_hbm, wv_hbm, hid_ref, gain_ref, out_ref,
    kqvg, wks, wvs, kg, vg,
    part, d2dr, acc, r1, fin, zs, zr, cs, cr, hs, hr, hg, gh, crossp, oown, osend,
    in_sem, w_sem, d2d_s, d2d_r, x_s, r1_r, fin_r, z_s, z_r, c_s, c_r,
    h_s, h_r, o_l, o_s, o_r,
):
    section = lax.axis_index("section")
    tensor = lax.axis_index("tensor")
    yh, x = lax.div(section, 4), lax.rem(section, 4)
    z, c = lax.div(tensor, 2), lax.rem(tensor, 2)
    xp, xm, x2 = lax.rem(x + 1, 4), lax.rem(x + 3, 4), lax.rem(x + 2, 4)
    me = yh * 8 + z
    me32 = yh * 16 + tensor
    to_core = {"tensor": z * 2 + (1 - c)}
    to_xp = {"section": yh * 4 + xp}
    to_xm = {"section": yh * 4 + xm}
    to_y = {"section": (1 - yh) * 4 + x}

    def to_yz(n):
        return {"section": lax.div(n, 8) * 4 + x, "tensor": lax.rem(n, 8) * 2 + c}

    def each(n, f, start=0):
        def body(i, _):
            f(i)
            return 0

        lax.fori_loop(start, n, body, 0)

    def wait_bytes(ref, sem):
        pltpu.make_async_copy(ref, ref, sem).wait()

    def load(i):
        b, h = i // HEADS, i % HEADS
        cols = pl.ds(pl.multiple_of(h * DK, DK), DK)
        for n, src in enumerate((k_hbm, q_hbm, v_hbm, g_hbm)):
            pltpu.make_async_copy(src.at[0, b, :, cols], kqvg.at[i, n], in_sem.at[i]).start()

    wcopies = [
        pltpu.make_async_copy(wk_hbm.at[0], wks, w_sem.at[0]),
        pltpu.make_async_copy(wv_hbm.at[0], wvs, w_sem.at[1]),
    ]
    each(HEADS, load)

    barrier = pltpu.get_barrier_semaphore()
    for peer in (to_xp, to_xm):
        pl.semaphore_signal(barrier, inc=1, device_id=peer, device_id_type=MESH)

    def greet(d):
        to = lax.rem(me32 + d, 32)
        peer = {"section": lax.div(to, 16) * 4 + x, "tensor": lax.rem(to, 16)}
        pl.semaphore_signal(barrier, inc=1, device_id=peer, device_id_type=MESH)

    each(32, greet, 1)
    for copy in wcopies:
        copy.start()

    def send(src, dst, s, r, peer):
        return pltpu.make_async_remote_copy(
            src_ref=src, dst_ref=dst, send_sem=s, recv_sem=r, device_id=peer, device_id_type=MESH
        )

    def x_copy(b, j, n):
        a = acc.at[b, j]
        src, dst, r, peer = (
            (a.at[x2], r1.at[b, j, 0], r1_r.at[b, j, 0], to_xp),
            (a.at[4 + x2], r1.at[b, j, 1], r1_r.at[b, j, 1], to_xm),
            (a.at[4 + xp], fin.at[b, j, 0, 1], fin_r.at[b, j], to_xp),
            (a.at[xm], fin.at[b, j, 1, 0], fin_r.at[b, j], to_xm),
            (a.at[xp], fin.at[b, j, 0, 0], fin_r.at[b, j], to_xp),
            (a.at[4 + xm], fin.at[b, j, 1, 1], fin_r.at[b, j], to_xm),
        )[n]
        return send(src, dst, x_s, r, peer)

    def project(b, j):
        at = pl.ds(pl.multiple_of(j * CW, CW), CW)
        p = dot(kg[...], wks[at, :], NT) + dot(vg[...], wvs[at, :], NT)
        part[b, j] = p.reshape(8, 2, 32, CW)
        send(part.at[b, j, :, 1 - c], d2dr.at[b, j], d2d_s, d2d_r.at[b, j], to_core).start()

    def stage1(b, j):
        wait_bytes(d2dr.at[b, j], d2d_r.at[b, j])
        acc[b, j] = part[b, j, :, c] + d2dr[b, j]
        for n in range(2):
            x_copy(b, j, n).start()

    def stage1b(b, j):
        for n in range(2, 4):
            x_copy(b, j, n).start()

    def stage2(b, j):
        wait_bytes(r1.at[b, j, 0], r1_r.at[b, j, 0])
        acc[b, j, xp] = acc[b, j, xp] + r1[b, j, 0]
        x_copy(b, j, 4).start()
        wait_bytes(r1.at[b, j, 1], r1_r.at[b, j, 1])
        acc[b, j, 4 + xm] = acc[b, j, 4 + xm] + r1[b, j, 1]
        x_copy(b, j, 5).start()

    def stage3(b, j):
        wait_bytes(fin.at[b, j], fin_r.at[b, j])
        for k in range(2):
            h = (1 - yh) if k == 0 else yh
            total = acc[b, j, h * 4 + x] + fin[b, j, 0, h] + fin[b, j, 1, h]
            for n in range(CW // 128):
                zt = j * (CW // 128) + n
                to = h * 8 + zt
                block = total[:, n * 128 : (n + 1) * 128]
                zs[b, to] = block
                crossp[h, pl.ds(pl.multiple_of(b * 32, 32), 32), :] += block * gh[b, h, zt]

                @pl.when(to != me)
                def _():
                    send(zs.at[b, to], zr.at[b, me], z_s, z_r, to_yz(to)).start()

    def head(i):
        cols = pl.ds(pl.multiple_of((i % HEADS) * DK, DK), DK)
        scores = dot(kqvg[i, 0], kqvg[i, 1], NT)
        top = jnp.max(scores, axis=0, keepdims=True)
        shifted = jnp.exp(scores - top)
        probs = shifted * (1.0 / jnp.sum(shifted, axis=0, keepdims=True))
        probs_low = probs.astype(BF16)
        prob_grad = dot(kqvg[i, 2], kqvg[i, 3], NT)
        row_dot = jnp.sum(probs_low.astype(F32) * prob_grad, axis=0, keepdims=True)
        score_low = (probs * (prob_grad - row_dot)).astype(BF16)
        vg[:, cols] = dot(probs_low, kqvg[i, 3], NN).astype(BF16)
        kg[:, cols] = dot(score_low, kqvg[i, 1], NN).astype(BF16)

    def gather_hidden():
        gain8 = jnp.broadcast_to(gain_ref[...], (8, 64))
        for half in range(2):
            at = slice(half * 32, (half + 1) * 32)
            hs[half, :32] = jnp.concatenate([hid_ref[0, at], hid_ref[1, at]], axis=-1)
            hs[half, 32:] = jnp.concatenate([gain8, gain8], axis=-1)
        hr[me32] = hs[c]

        def start(d):
            to = lax.rem(me32 + d, 32)
            peer = {"section": lax.div(to, 16) * 4 + x, "tensor": lax.rem(to, 16)}
            send(hs.at[lax.rem(to, 2)], hr.at[me32], h_s, h_r, peer).start()

        each(32, start, 1)

    def take_hidden():
        wait_bytes(hr.at[pl.ds(0, 31)], h_r)
        low = lax.broadcasted_iota(jnp.int32, (40, 128), 1) < 64
        for h in range(2):
            for zt in range(8):
                even, odd = hr[h * 16 + 2 * zt], hr[h * 16 + 2 * zt + 1]
                first = jnp.where(low, even, pltpu.roll(odd, 64, 1))
                second = jnp.where(low, pltpu.roll(even, 64, 1), odd)
                gain_row = first[32:33]
                for b, hidden in enumerate((first[:32], second[:32])):
                    hg[h, zt, b * 32 : (b + 1) * 32] = hidden
                    gh[b, h, zt] = hidden * gain_row
                hg[h, zt, 64:72] = first[32:]
        crossp[...] = jnp.zeros_like(crossp)

    def group(n):
        @pl.when(n == 1)
        def _():
            pl.semaphore_wait(barrier, 33)
            gather_hidden()

        @pl.when(n == HEADS // GROUP)
        def _():
            for copy in wcopies:
                copy.wait()

            def first(t):
                @pl.when(t < NJ)
                def _():
                    project(0, t)

                @pl.when(t >= 2)
                def _():
                    stage1(0, t - 2)

            each(NJ + 2, first)
            each(NJ, lambda j: stage1b(0, j))

        @pl.when(n == HEADS // GROUP + 1)
        def _():
            each(NJ, lambda j: stage2(0, j))

        @pl.when(n < HEADS // GROUP)
        def _():
            each((n + 1) * GROUP + HEADS, load, n * GROUP + HEADS)

        for k in range(GROUP):
            wait_bytes(kqvg.at[n * GROUP + k], in_sem.at[n * GROUP + k])
        for k in range(GROUP):
            head(n * GROUP + k)

    each(NSEQ * HEADS // GROUP, group)

    def tail(t):
        @pl.when(t < NJ)
        def _():
            project(1, t)

        @pl.when((t >= 2) & (t < NJ + 2))
        def _():
            stage1(1, t - 2)
            stage1b(1, t - 2)

        @pl.when(t == 3)
        def _():
            take_hidden()
            each(NJ, lambda j: stage3(0, j))

        @pl.when((t >= 3) & (t < NJ + 3))
        def _():
            stage2(1, t - 3)

        @pl.when(t >= 5)
        def _():
            stage3(1, t - 5)

    each(NJ + 5, tail)

    for h in range(2):
        cs[h] = dot(jnp.ones((8, 128), F32), crossp[h], NT, precision=lax.Precision.HIGHEST)

    def start_cross(d):
        to = lax.rem(me + d, 16)
        send(cs.at[lax.div(to, 8)], cr.at[me], c_s, c_r, to_yz(to)).start()

    each(16, start_cross, 1)

    hid_mine, gain_mine = hg[yh, z, :64], hg[yh, z, 64:65]
    square = jnp.zeros((64, 128), F32)
    for zt in range(8):
        hidden = hg[yh, zt, :64]
        square = square + hidden * hidden
    square = jnp.sum(square, axis=-1, keepdims=True)
    inverse = lax.rsqrt(square * (1.0 / D) + EPS)

    def finish():
        wait_bytes(zr.at[:, pl.ds(0, 15)], z_r)
        wait_bytes(cr.at[pl.ds(0, 15)], c_r)

    finish()
    for b in range(NSEQ):
        zr[b, me] = zs[b, me]
    cr[me] = cs[yh]
    cross = cr[0]
    for t in range(1, 16):
        cross = cross + cr[t]
    wide = jnp.broadcast_to(cross[:1], (64, 128))
    row = lax.broadcasted_iota(jnp.int32, (64, 128), 0)
    lane = lax.broadcasted_iota(jnp.int32, (64, 128), 1)
    cross_col = jnp.sum(jnp.where(row == lane, wide, 0.0), axis=-1, keepdims=True)
    scale = cross_col * inverse * inverse * inverse * (1.0 / D)
    for b in range(NSEQ):
        at = slice(b * 32, (b + 1) * 32)
        grad = zr[b, 0]
        for t in range(1, 16):
            grad = grad + zr[b, t]
        done = gain_mine * grad * inverse[at] - hid_mine[at] * scale[at]
        oown[b] = jnp.where(c == 0, done[:, :64], done[:, 64:])
        osend[b] = jnp.where(c == 0, done[:, 64:], done[:, :64])
    half = out_ref.at[:, pl.ds(pl.multiple_of(c * 32, 32), 32), :]
    other = out_ref.at[:, pl.ds(pl.multiple_of((1 - c) * 32, 32), 32), :]
    away = send(osend, half, o_s, o_r, to_core)
    away.start()
    here = pltpu.make_async_copy(oown, half, o_l)
    here.start()

    wait_bytes(d2dr, d2d_s)
    wait_bytes(acc.at[:, :, pl.ds(0, 6)], x_s)
    wait_bytes(zs.at[:, pl.ds(0, 15)], z_s)
    wait_bytes(cr.at[pl.ds(0, 15)], c_s)
    wait_bytes(hr.at[pl.ds(0, 31)], h_s)
    here.wait()
    away.wait_send()
    wait_bytes(other, o_r)


def per_device(q, k, v, g, wk, wv, hidden, gain):
    dma = pltpu.SemaphoreType.DMA
    vm = pltpu.VMEM
    hbm = pl.BlockSpec(memory_space=pltpu.HBM)
    vmem = pl.BlockSpec(memory_space=pltpu.VMEM)
    return pl.pallas_call(
        kernel,
        out_shape=jax.ShapeDtypeStruct((NSEQ, 64, 64), F32),
        in_specs=[hbm] * 6 + [vmem] * 2,
        out_specs=vmem,
        scratch_shapes=[
            vm((NSEQ * HEADS, 4, ROWS, DK), BF16),
            vm((D, D), BF16), vm((D, D), BF16),
            vm((ROWS, D), BF16), vm((ROWS, D), BF16),
            vm((NSEQ, NJ, 8, 2, 32, CW), F32),
            vm((NSEQ, NJ, 8, 32, CW), F32),
            vm((NSEQ, NJ, 8, 32, CW), F32),
            vm((NSEQ, NJ, 2, 32, CW), F32),
            vm((NSEQ, NJ, 2, 2, 32, CW), F32),
            vm((NSEQ, 16, 32, 128), F32),
            vm((NSEQ, 16, 32, 128), F32),
            vm((2, 8, 128), F32),
            vm((16, 8, 128), F32),
            vm((2, 40, 128), F32),
            vm((32, 40, 128), F32),
            vm((2, 8, 72, 128), F32),
            vm((NSEQ, 2, 8, 32, 128), F32),
            vm((2, 128, 128), F32),
            vm((NSEQ, 32, 64), F32),
            vm((NSEQ, 32, 64), F32),
            dma((NSEQ * HEADS,)), dma((2,)),
            dma, dma((NSEQ, NJ)),
            dma, dma((NSEQ, NJ, 2)), dma((NSEQ, NJ)),
            dma, dma,
            dma, dma,
            dma, dma,
            dma, dma, dma,
        ],
        compiler_params=pltpu.CompilerParams(
            collective_id=0,
            has_side_effects=True,
            vmem_limit_bytes=55136 * 1024,

        ),
    )(q, k, v, g, wk, wv, hidden, gain.reshape(1, 64))


def solution(mesh):
    return jax.shard_map(
        per_device,
        mesh=mesh,
        in_specs=(
            P("section", "dp", None, "tensor"),
            P("section", "dp", None, "tensor"),
            P("section", "dp", None, "tensor"),
            P("section", "dp", None, "tensor"),
            P("section", None, "tensor"),
            P("section", None, "tensor"),
            P("dp", "section", "tensor"),
            P("tensor"),
        ),
        out_specs=P("dp", "section", "tensor"),
        check_vma=False,
    )
```
